32 devices in a mesh: node: 32 (over z, y, x, core).
Axes of the slice: x: 2, y: 2, z: 4, core: 2. Of those that a mesh axis runs over, the one named last changes fastest.
Arguments:
- labels: bfloat16 [131072, 512], P('node'), may hold values from -6 to 6
- seed_mask: int32 [131072], P('node'), may hold values 0 or 1
- band_w: bfloat16 [1024, 3, 128, 128], P('node'), may hold values from 0.0009994507 to 1
- far_block: int32 [32, 32, 2], P('node'), may hold values from 0 to 511
- far_tile: int32 [32, 32, 2], P('node'), may hold values from 0 to 31
- far_count: int32 [32, 32], P('node'), may hold values from 0 to 2, as said below
- far_w: bfloat16 [32, 32, 2, 8, 128], P('node'), may hold values from 0.049804688 to 2
Outputs:
- final_labels: bfloat16 [131072, 512], P('node')
- residual: float32 [2, 1024], P(None, 'node')
The draws below stay inside these ranges and needn't reach their ends.
Inputs may be any that keep to these rules, and one draw needn't show every extreme that they name: `far_count`: in every draw at least one destination shard has all 2 slots live from every source shard; other counts vary from pair to pair.
All inputs are finite; a program needn't handle non-finite values. No bound on the sum of `seed_mask` on one device may be relied on, other than what follows from the above.
Results may differ from the reference program's by a relative error of at most 0.0027.
Values may be sent and summed in bfloat16 or wider, within the bound.
A program may use at most 128 MiB of HBM per device.

```python
import math
import jax
import jax.numpy as jnp
from jax import lax

C = 512
NODE_DEV = 4096
TILE = 128
BLK = 8
SLOTS = 2
ITERS = 2
NODES = 131072
N_NODE = 32


def draw_far_count(key, part):
    first_key, second_key = jax.random.split(jax.random.fold_in(key, 17))
    counts = jax.random.randint(first_key, (N_NODE, N_NODE), 0, SLOTS + 1)
    busiest = jax.random.randint(second_key, (), 0, N_NODE)
    row_ids = jnp.arange(N_NODE)[:, None]
    return jnp.where(row_ids == busiest, SLOTS, counts).astype(jnp.int32)


def set_ends(values, rng, smallest, top_value):
    dims = values.shape
    place = [jax.random.randint(jax.random.fold_in(rng, axis), (), 0, dims[axis]) for axis in range(len(dims))]
    values = values.at[tuple(place)].set(smallest)
    longest = dims.index(max(dims))
    place[longest] = (place[longest] + 1) % dims[longest]
    return values.at[tuple(place)].set(top_value)


def block_scale(own_key, dims, cuts, smallest, high):
    factor_of, own = 1.0, jax.random.fold_in(own_key, 6)
    for dim, parts in cuts:
        steps = jnp.exp(jax.random.uniform(jax.random.fold_in(own, dim), (parts,), jnp.float32, smallest / len(cuts), high / len(cuts)))
        factor_of = factor_of * jnp.repeat(steps, dims[dim] // parts).reshape([-1 if axis == dim else 1 for axis in range(len(dims))])
    return factor_of


def normal_values(own_key, shape, width, most, pieces=(), dtype=jnp.bfloat16):
    array = width * jax.random.normal(own_key, shape, jnp.float32)
    if pieces:
        array = array * block_scale(own_key, shape, pieces, -0.22, 0.18)
    return jnp.clip(array, -most, most).astype(dtype)


def setup_inputs(seed: int = 0) -> dict:
    key_of = jax.random.split(jax.random.key(seed), 8)
    return {
        "labels": normal_values(key_of[0], (NODES, C), 1.0, 6.0, ((0, 32),)),
        "seed_mask": set_ends((jax.random.randint(key_of[1], (NODES,), 0, 4) < 1).astype(jnp.int32), jax.random.fold_in(key_of[1], 1), 0, 1),
        "band_w": jnp.clip(jnp.exp(math.log(1.0) - 6.9083047 * jax.random.uniform(key_of[2], (NODES // TILE, 3, TILE, TILE), jnp.float32) ** block_scale(key_of[2], (NODES // TILE, 3, TILE, TILE), ((0, 32),), -0.2, 0.2)), 0.0009994507, 1.0).astype(jnp.bfloat16),
        "far_block": set_ends(jax.random.randint(key_of[3], (N_NODE, N_NODE, SLOTS), 0, NODE_DEV // BLK), jax.random.fold_in(key_of[3], 1), 0, (NODE_DEV // BLK) - 1).astype(jnp.int32),
        "far_tile": set_ends(jax.random.randint(key_of[4], (N_NODE, N_NODE, SLOTS), 0, NODE_DEV // TILE), jax.random.fold_in(key_of[4], 1), 0, (NODE_DEV // TILE) - 1).astype(jnp.int32),
        "far_count": draw_far_count(jax.random.fold_in(key_of[7], 71), 0),
        "far_w": jnp.clip(jnp.exp(math.log(2.0) - 3.6927934 * jax.random.uniform(key_of[6], (N_NODE, N_NODE, SLOTS, BLK, TILE), jnp.float32) ** block_scale(key_of[6], (N_NODE, N_NODE, SLOTS, BLK, TILE), ((0, 32),), -0.2, 0.2)), 0.049804688, 2.0).astype(jnp.bfloat16),
    }


def live_table(count_row):
    return (jnp.arange(SLOTS)[None, :] < count_row[:, None]).astype(jnp.float32)

def reference(labels, seed_mask, band_w, far_block, far_tile, far_count, far_w):
    tile_total = labels.shape[0] // TILE
    block_count = NODE_DEV // BLK
    band_wide = band_w.astype(jnp.float32)
    degree_band = lax.optimization_barrier(jnp.sum(band_wide, axis=(1, 3)))

    def far_degree(packed):
        tiles_here, count_here, weight_here = packed
        live_weights = weight_here.astype(jnp.float32) * live_table(count_here)[:, :, None, None]
        weight_sums = lax.optimization_barrier(jnp.sum(live_weights, axis=2)).reshape(-1, TILE)
        return jnp.zeros((NODE_DEV // TILE, TILE), jnp.float32).at[tiles_here.reshape(-1)].add(weight_sums)
    degree_far = lax.map(far_degree, (far_tile, far_count, far_w)).reshape(tile_total, TILE)
    degree = degree_band + degree_far
    seeded = (seed_mask == 1).reshape(tile_total, TILE, 1)
    clamped = labels.astype(jnp.float32).reshape(tile_total, TILE, C)
    current = labels
    residuals = []
    for sweep in range(ITERS):
        tiles = current.astype(jnp.float32).reshape(tile_total, TILE, C)
        band_sum = jnp.zeros((tile_total, TILE, C), jnp.float32)
        for offset in (-1, 0, 1):
            source = jnp.roll(tiles, -offset, axis=0)
            band_sum = band_sum + jnp.einsum('itr,irc->itc', band_wide[:, offset + 1], source)
        blocks_all = current.reshape(N_NODE, block_count, BLK, C)

        def far_part(packed):
            wanted, tiles_here, count_here, weight_here = packed
            blocks = blocks_all[jnp.arange(N_NODE)[:, None], wanted].astype(jnp.float32)
            live_weights = weight_here.astype(jnp.float32) * live_table(count_here)[:, :, None, None]
            contrib = jnp.einsum('skqt,skqc->sktc', live_weights, blocks)
            return jnp.zeros((NODE_DEV // TILE, TILE, C), jnp.float32).at[tiles_here.reshape(-1)].add(contrib.reshape(-1, TILE, C))
        far_sum = lax.map(far_part, (far_block, far_tile, far_count, far_w)).reshape(tile_total, TILE, C)
        averaged = (band_sum + far_sum) / degree[:, :, None]
        row_scale = jnp.sqrt(lax.optimization_barrier(jnp.mean(averaged * averaged, axis=2, keepdims=True)))
        scaled = averaged / jnp.maximum(row_scale, 0.05)
        fresh = jnp.where(seeded, clamped, scaled).astype(jnp.bfloat16)
        residuals.append(lax.optimization_barrier(jnp.sum(jnp.abs(fresh.astype(jnp.float32) - tiles), axis=(1, 2))))
        current = fresh.reshape(labels.shape[0], C)
    return (current, jnp.stack(residuals))
```

```python
import functools

import jax
import jax.numpy as jnp
from jax import lax
from jax.experimental import pallas as pl
from jax.experimental.pallas import tpu as pltpu
from jax.sharding import PartitionSpec as P

ITERS = 2
MESH = pl.DeviceIdType.MESH
ROWS = 32
GROUP = 16


def kernel(
    dims,
    labels_hbm, band_hbm, farw_hbm, req_ref, slot_ref, seed_ref,
    out_hbm, res_ref,
    cur0, cur1, band, farw, wide_t, onehot, placed, acc, inv, part,
    halo0, halo1, send0, send1, recv0, recv1, req_in, req_s,
    lab_sem, band_sem, farw_sem, smem_sem, out_sem,
    req_send, req_recv, halo_send, halo_recv, blk_send, blk_recv,
):
    n, tiles, tile, slots, blk, classes = dims
    rows = tiles * tile
    lane = 128
    per = slots * blk
    far_rows = n * per
    me = lax.axis_index("node")
    right, left = lax.rem(me + 1, n), lax.rem(me + n - 1, n)
    cur = (cur0, cur1)
    halo, send, recv = (halo0, halo1), (send0, send1), (recv0, recv1)

    def groups(start, size):
        return pl.ds(start // GROUP, size // GROUP)

    def as_rows(value):
        return value.reshape(-1, classes)

    lab_copy = pltpu.make_async_copy(labels_hbm, cur0.at[groups(tile, rows)], lab_sem)
    band_copy = pltpu.make_async_copy(band_hbm, band, band_sem)
    farw_copy = pltpu.make_async_copy(farw_hbm, farw, farw_sem)
    lab_copy.start()
    farw_copy.start()
    band_copy.start()

    barrier = pltpu.get_barrier_semaphore()

    @pl.loop(1, n)
    def _(j):
        pl.semaphore_signal(barrier, inc=1, device_id=(lax.rem(me + j, n),), device_id_type=MESH)

    pl.semaphore_wait(barrier, n - 1)

    @pl.loop(1, n)
    def _(j):
        peer = lax.rem(me + j, n)
        pltpu.make_async_remote_copy(
            req_ref.at[peer], req_in.at[me], req_send, req_recv,
            device_id=(peer,), device_id_type=MESH,
        ).start()

    def halo_copies(it, low, high):
        return (
            pltpu.make_async_remote_copy(
                high, halo[it].at[0], halo_send.at[it, 0], halo_recv.at[it, 0],
                device_id=(right,), device_id_type=MESH,
            ),
            pltpu.make_async_remote_copy(
                low, halo[it].at[1], halo_send.at[it, 1], halo_recv.at[it, 1],
                device_id=(left,), device_id_type=MESH,
            ),
        )

    halo_first = halo_copies(
        0, labels_hbm.at[groups(0, tile)], labels_hbm.at[groups(rows - tile, tile)]
    )
    for copy in halo_first:
        copy.start()

    req_in[me] = req_ref[me]
    lab_copy.wait()
    pltpu.make_async_copy(req_in.at[pl.ds(0, n - 1)], req_in.at[pl.ds(0, n - 1)], req_recv).wait()
    smem_copy = pltpu.make_async_copy(req_in, req_s, smem_sem)
    smem_copy.start()
    smem_copy.wait()

    def block_copy(it, j):
        peer = lax.rem(me + j, n)
        return pltpu.make_async_remote_copy(
            send[it].at[peer], recv[it].at[me], blk_send.at[it], blk_recv.at[it],
            device_id=(peer,), device_id_type=MESH,
        )

    def gathered(it, peer):
        halves = []
        for k in range(slots):
            wanted = req_s[peer, 0, k]
            pair = cur[it][wanted // 2 + tile // GROUP].astype(jnp.float32)
            odd = jnp.full((blk, classes), wanted % 2, jnp.int32) == 1
            halves.append(jnp.where(odd, pair[blk:], pair[:blk]))
        return jnp.concatenate(halves, axis=0).astype(jnp.bfloat16)

    def exchange(it):
        @pl.loop(1, n)
        def _(j):
            peer = lax.rem(me + j, n)
            send[it][peer] = gathered(it, peer)

            @pl.when(j > 1)
            def _():
                block_copy(it, j - 1).start()

        recv[it][me] = gathered(it, me)
        block_copy(it, n - 1).start()

    def await_halo(it, copies):
        for copy in copies:
            copy.wait()
        cur[it][groups(0, tile)] = halo[it][0]
        cur[it][groups(rows + tile, tile)] = halo[it][1]

    def await_blocks(it):
        both = pl.ds(0, n - 1)
        pltpu.make_async_copy(send[it].at[both], send[it].at[both], blk_send.at[it]).wait()
        pltpu.make_async_copy(recv[it].at[both], recv[it].at[both], blk_recv.at[it]).wait()

    def band_pass(it):
        zero = jnp.zeros((tile, tile), jnp.bfloat16)

        @pl.loop(0, tiles // 2)
        def _(p):
            first = [band[2 * p, o] for o in range(3)]
            second = [band[2 * p + 1, o] for o in range(3)]
            weights = jnp.concatenate(
                [jnp.concatenate(first + [zero], axis=1), jnp.concatenate([zero] + second, axis=1)],
                axis=0,
            )
            base = pl.multiple_of(p * (2 * tile), 2 * tile)
            acc[pl.ds(base, 2 * tile), :] = jnp.dot(
                weights,
                as_rows(cur[it][pl.ds(p * (2 * tile // GROUP), 4 * tile // GROUP)]),
                preferred_element_type=jnp.float32,
            )

    def far_pass(it, p):
        base = pl.multiple_of(p * (2 * tile), 2 * tile)
        acc[pl.ds(base, 2 * tile), :] += jnp.dot(
            placed[pl.ds(base, 2 * tile), :],
            recv[it][...].reshape(far_rows, classes),
            preferred_element_type=jnp.float32,
        )

    def finish(it, p):
        target = cur[1 - it]
        for half in range(2):
            total = jnp.zeros((8, lane), jnp.float32)
            for r in range(0, tile, ROWS):
                base = pl.multiple_of(p * (2 * tile) + half * tile + r, ROWS)
                here = pl.ds(base, ROWS)
                spread = [acc[here, c : c + lane] for c in range(0, classes, lane)]
                squares = spread[0] * spread[0]
                for s in spread[1:]:
                    squares = squares + s * s
                mean = jnp.sum(squares, axis=1, keepdims=True) * (1.0 / classes)
                signed = inv[here, :]
                size = jnp.abs(signed)
                factor = size / jnp.maximum(size * jnp.sqrt(mean), 0.05)
                keep = signed < 0.0
                padded = pl.ds(
                    p * (2 * tile // GROUP) + (half * tile + r + tile) // GROUP, ROWS // GROUP
                )
                for q, s in enumerate(spread):
                    where = slice(q * lane, (q + 1) * lane)
                    before = cur[it][padded, :, where].reshape(ROWS, lane).astype(jnp.float32)
                    fresh = jnp.where(keep, before, s * factor).astype(jnp.bfloat16)
                    target[padded, :, where] = fresh.reshape(ROWS // GROUP, GROUP, lane)
                    change = jnp.abs(fresh.astype(jnp.float32) - before)
                    for i in range(0, ROWS, 8):
                        total = total + change[i : i + 8]
            part[2 * p + half] = total

    def prepare():
        wide_t[...] = farw[...].astype(jnp.float32).T
        count = slot_ref.shape[1]
        chosen = slot_ref[...] == lax.broadcasted_iota(jnp.int32, (tiles, count), 0)
        slot_of = lax.shift_right_logical(
            lax.broadcasted_iota(jnp.int32, (count, far_rows), 1), blk.bit_length() - 1
        )
        spread = slot_of == lax.broadcasted_iota(jnp.int32, (count, far_rows), 0)
        onehot[...] = jnp.dot(
            chosen.astype(jnp.float32).astype(jnp.bfloat16),
            spread.astype(jnp.float32).astype(jnp.bfloat16),
            preferred_element_type=jnp.float32,
        )

        @pl.loop(0, tiles)
        def _(t):
            base = pl.multiple_of(t * tile, tile)
            weights = wide_t[...] * onehot[pl.ds(t, 1), :]
            placed[pl.ds(base, tile), :] = weights.astype(jnp.bfloat16)
            total = band[t, 0].astype(jnp.float32)
            for o in range(1, 3):
                total = total + band[t, o].astype(jnp.float32)
            for c in range(0, far_rows, lane):
                total = total + weights[:, c : c + lane]
            degree = jnp.sum(total, axis=1, keepdims=True)
            seeded = jnp.broadcast_to(seed_ref[pl.ds(t, 1), :].astype(jnp.float32), (tile, tile)).T
            inverse = jnp.broadcast_to(1.0 / degree, (tile, tile))
            inv[pl.ds(base, tile), :] = jnp.where(seeded == 1.0, -inverse, inverse)

    def out_copy(p):
        base = p * (2 * tile // GROUP)
        return pltpu.make_async_copy(
            cur[ITERS % 2].at[pl.ds(base + tile // GROUP, 2 * tile // GROUP)],
            out_hbm.at[pl.ds(base, 2 * tile // GROUP)],
            out_sem,
        )

    for it in range(ITERS):
        if it:
            copies = halo_copies(
                it, cur[it].at[groups(tile, tile)], cur[it].at[groups(rows, tile)]
            )
        else:
            copies = halo_first
        exchange(it)
        if it:
            for copy in copies:
                copy.start()
        else:
            farw_copy.wait()
            band_copy.wait()
            prepare()
        await_halo(it, copies)
        band_pass(it)
        await_blocks(it)

        last = it == ITERS - 1

        @pl.loop(0, tiles // 2)
        def _(p):
            far_pass(it, p)
            finish(it, p)
            if last:

                @pl.when(p > 0)
                def _():
                    out_copy(p - 1).start()

        sums = jnp.sum(part[...], axis=1)
        res_ref[it : it + 1, :] = jnp.sum(sums.T, axis=0, keepdims=True)

    out_copy(tiles // 2 - 1).start()
    whole = pltpu.make_async_copy(cur[ITERS % 2].at[groups(tile, rows)], out_hbm, out_sem)
    whole.wait()
    both = pl.ds(0, n - 1)
    pltpu.make_async_copy(req_ref.at[both], req_ref.at[both], req_send).wait()


def body(labels, seed_mask, band_w, far_block, far_tile, far_count, far_w):
    rows, classes = labels.shape
    tiles, _, tile, _ = band_w.shape
    _, n, slots, blk, _ = far_w.shape
    lane = 128
    per = slots * blk
    live = jnp.arange(slots, dtype=jnp.int32)[None, :] < far_count[0][:, None]
    slot_tile = jnp.where(live, far_tile[0], -1).reshape(1, n * slots)
    requests = jnp.pad(far_block[0], ((0, 0), (0, lane - slots))).reshape(n, 1, lane)
    dims = (n, tiles, tile, slots, blk, classes)
    vmem, anywhere = pltpu.VMEM, pl.BlockSpec(memory_space=pl.ANY)
    held = pl.BlockSpec(memory_space=pltpu.VMEM)
    dma = pltpu.SemaphoreType.DMA
    bf16, f32 = jnp.bfloat16, jnp.float32
    out, residual = pl.pallas_call(
        functools.partial(kernel, dims),
        out_shape=(
            jax.ShapeDtypeStruct((rows // GROUP, GROUP, classes), bf16),
            jax.ShapeDtypeStruct((ITERS, tiles), f32),
        ),
        in_specs=[anywhere, anywhere, anywhere, held, held, held],
        out_specs=(anywhere, held),
        scratch_shapes=[
            vmem(((rows + 2 * tile) // GROUP, GROUP, classes), bf16),
            vmem(((rows + 2 * tile) // GROUP, GROUP, classes), bf16),
            vmem(band_w.shape, bf16),
            vmem((n * per, tile), bf16),
            vmem((tile, n * per), f32),
            vmem((tiles, n * per), f32),
            vmem((rows, n * per), bf16),
            vmem((rows, classes), f32),
            vmem((rows, lane), f32),
            vmem((tiles, 8, lane), f32),
            vmem((2, tile // GROUP, GROUP, classes), bf16),
            vmem((2, tile // GROUP, GROUP, classes), bf16),
            vmem((n, per, classes), bf16),
            vmem((n, per, classes), bf16),
            vmem((n, per, classes), bf16),
            vmem((n, per, classes), bf16),
            vmem((n, 1, lane), jnp.int32),
            pltpu.SMEM((n, 1, lane), jnp.int32),
            dma, dma, dma, dma, dma,
            dma, dma,
            dma((ITERS, 2)), dma((ITERS, 2)),
            dma((ITERS,)), dma((ITERS,)),
        ],
        compiler_params=pltpu.CompilerParams(
            collective_id=0, has_side_effects=True, vmem_limit_bytes=60 * 1024 * 1024
        ),
    )(
        labels.reshape(rows // GROUP, GROUP, classes),
        band_w,
        far_w.reshape(n * per, tile),
        requests,
        slot_tile,
        seed_mask.reshape(tiles, tile),
    )
    return out.reshape(rows, classes), residual


def solution(mesh):
    placed = (
        P("node", None),
        P("node"),
        P("node", None, None, None),
        P("node", None, None),
        P("node", None, None),
        P("node", None),
        P("node", None, None, None, None),
    )
    return jax.shard_map(
        body,
        mesh=mesh,
        in_specs=placed,
        out_specs=(P("node", None), P(None, "node")),
        check_vma=False,
    )
```

```python
import functools

import jax
import jax.numpy as jnp
from jax import lax
from jax.experimental import pallas as pl
from jax.experimental.pallas import tpu as pltpu
from jax.sharding import PartitionSpec as P

ITERS = 2
MESH = pl.DeviceIdType.MESH
ROWS = 32
GROUP = 16


def kernel(
    dims,
    labels_hbm, band_hbm, farw_hbm, req_ref, tile_ref, count_ref, seed_ref,
    out_hbm, res_ref,
    cur0, cur1, band, farw, wide_t, onehot, placed, acc, far_a, far_b, inv, part,
    halo0, halo1, send0, send1, recv0, recv1, req_in, req_s,
    lab_sem, band_sem, farw_sem, smem_sem, out_sem,
    req_send, req_recv, halo_send, halo_recv, blk_send, blk_recv,
):
    n, tiles, tile, slots, blk, classes = dims
    rows = tiles * tile
    lane = 128
    per = slots * blk
    far_rows = n * per
    me = lax.axis_index("node")
    right, left = lax.rem(me + 1, n), lax.rem(me + n - 1, n)
    cur = (cur0, cur1)
    halo, send, recv = (halo0, halo1), (send0, send1), (recv0, recv1)

    def groups(start, size):
        return pl.ds(start // GROUP, size // GROUP)

    def as_rows(value):
        return value.reshape(-1, classes)

    lab_copy = pltpu.make_async_copy(labels_hbm, cur0.at[groups(tile, rows)], lab_sem)
    band_copy = pltpu.make_async_copy(band_hbm, band, band_sem)
    farw_copy = pltpu.make_async_copy(farw_hbm, farw, farw_sem)
    lab_copy.start()
    farw_copy.start()
    band_copy.start()

    barrier = pltpu.get_barrier_semaphore()

    @pl.loop(1, n)
    def _(j):
        pl.semaphore_signal(barrier, inc=1, device_id=(lax.rem(me + j, n),), device_id_type=MESH)

    pl.semaphore_wait(barrier, n - 1)

    @pl.loop(1, n)
    def _(j):
        peer = lax.rem(me + j, n)
        pltpu.make_async_remote_copy(
            req_ref, req_in.at[me], req_send, req_recv,
            device_id=(peer,), device_id_type=MESH,
        ).start()

    def halo_copies(it, low, high):
        return (
            pltpu.make_async_remote_copy(
                high, halo[it].at[0], halo_send.at[it, 0], halo_recv.at[it, 0],
                device_id=(right,), device_id_type=MESH,
            ),
            pltpu.make_async_remote_copy(
                low, halo[it].at[1], halo_send.at[it, 1], halo_recv.at[it, 1],
                device_id=(left,), device_id_type=MESH,
            ),
        )

    halo_first = halo_copies(
        0, labels_hbm.at[groups(0, tile)], labels_hbm.at[groups(rows - tile, tile)]
    )
    for copy in halo_first:
        copy.start()

    req_in[me] = req_ref[...]
    lab_copy.wait()
    pltpu.make_async_copy(req_in.at[pl.ds(0, n - 1)], req_in.at[pl.ds(0, n - 1)], req_recv).wait()
    smem_copy = pltpu.make_async_copy(req_in, req_s, smem_sem)
    smem_copy.start()
    smem_copy.wait()

    def block_copy(it, j):
        peer = lax.rem(me + j, n)
        return pltpu.make_async_remote_copy(
            send[it].at[peer], recv[it].at[me], blk_send.at[it], blk_recv.at[it],
            device_id=(peer,), device_id_type=MESH,
        )

    def gathered(it, peer):
        halves = []
        for k in range(slots):
            wanted = req_s[peer, k, me]
            pair = cur[it][wanted // 2 + tile // GROUP].astype(jnp.float32)
            odd = jnp.full((blk, classes), wanted % 2, jnp.int32) == 1
            halves.append(jnp.where(odd, pair[blk:], pair[:blk]))
        return jnp.concatenate(halves, axis=0).astype(jnp.bfloat16)

    def exchange(it):
        @pl.loop(1, n)
        def _(j):
            peer = lax.rem(me + j, n)
            send[it][peer] = gathered(it, peer)

            @pl.when(j > 1)
            def _():
                block_copy(it, j - 1).start()

        recv[it][me] = gathered(it, me)
        block_copy(it, n - 1).start()

    def await_halo(it, copies):
        for copy in copies:
            copy.wait()
        cur[it][groups(0, tile)] = halo[it][0]
        cur[it][groups(rows + tile, tile)] = halo[it][1]

    def await_blocks(it):
        both = pl.ds(0, n - 1)
        pltpu.make_async_copy(send[it].at[both], send[it].at[both], blk_send.at[it]).wait()
        pltpu.make_async_copy(recv[it].at[both], recv[it].at[both], blk_recv.at[it]).wait()

    def band_pass(it, start, stop):
        zero = jnp.zeros((tile, tile), jnp.bfloat16)

        @pl.loop(start, stop)
        def _(p):
            first = [band[2 * p, o] for o in range(3)]
            second = [band[2 * p + 1, o] for o in range(3)]
            weights = jnp.concatenate(
                [jnp.concatenate(first + [zero], axis=1), jnp.concatenate([zero] + second, axis=1)],
                axis=0,
            )
            base = pl.multiple_of(p * (2 * tile), 2 * tile)
            acc[pl.ds(base, 2 * tile), :] = jnp.dot(
                weights,
                as_rows(cur[it][pl.ds(p * (2 * tile // GROUP), 4 * tile // GROUP)]),
                preferred_element_type=jnp.float32,
            )

    def far_pass(it, p, into):
        base = pl.multiple_of(p * (2 * tile), 2 * tile)
        into[...] = jnp.dot(
            placed[pl.ds(base, 2 * tile), :],
            recv[it][...].reshape(far_rows, classes),
            preferred_element_type=jnp.float32,
        )

    def finish(it, p, far):
        target = cur[1 - it]
        for half in range(2):
            total = jnp.zeros((8, lane), jnp.float32)
            for r in range(0, tile, ROWS):
                base = pl.multiple_of(p * (2 * tile) + half * tile + r, ROWS)
                here = pl.ds(base, ROWS)
                local = slice(half * tile + r, half * tile + r + ROWS)
                spread = [
                    acc[here, c : c + lane] + far[local, c : c + lane]
                    for c in range(0, classes, lane)
                ]
                squares = spread[0] * spread[0]
                for s in spread[1:]:
                    squares = squares + s * s
                mean = jnp.sum(squares, axis=1, keepdims=True) * (1.0 / classes)
                signed = inv[here, :]
                size = jnp.abs(signed)
                factor = size / jnp.maximum(size * jnp.sqrt(mean), 0.05)
                keep = signed < 0.0
                padded = pl.ds(
                    p * (2 * tile // GROUP) + (half * tile + r + tile) // GROUP, ROWS // GROUP
                )
                for q, s in enumerate(spread):
                    where = slice(q * lane, (q + 1) * lane)
                    before = cur[it][padded, :, where].reshape(ROWS, lane).astype(jnp.float32)
                    fresh = jnp.where(keep, before, s * factor).astype(jnp.bfloat16)
                    target[padded, :, where] = fresh.reshape(ROWS // GROUP, GROUP, lane)
                    change = jnp.abs(fresh.astype(jnp.float32) - before)
                    for i in range(0, ROWS, 8):
                        total = total + change[i : i + 8]
            part[2 * p + half] = total

    def prepare():
        wide_t[...] = farw[...].astype(jnp.float32).T
        tile_of = lax.broadcasted_iota(jnp.int32, (tiles, n), 0)
        block_of = lax.shift_right_logical(
            lax.broadcasted_iota(jnp.int32, (n, far_rows), 1), blk.bit_length() - 1
        )
        peer_of = lax.broadcasted_iota(jnp.int32, (n, far_rows), 0)
        table = jnp.zeros((tiles, far_rows), jnp.float32)
        for k in range(slots):
            target = jnp.where(count_ref[...] > k, tile_ref[k : k + 1, :], -1)
            chosen = (tile_of == target).astype(jnp.float32)
            spread = (block_of == peer_of * slots + k).astype(jnp.float32)
            table = table + jnp.dot(
                chosen.astype(jnp.bfloat16),
                spread.astype(jnp.bfloat16),
                preferred_element_type=jnp.float32,
            )
        onehot[...] = table

        @pl.loop(0, tiles)
        def _(t):
            base = pl.multiple_of(t * tile, tile)
            weights = wide_t[...] * onehot[pl.ds(t, 1), :]
            placed[pl.ds(base, tile), :] = weights.astype(jnp.bfloat16)
            total = band[t, 0].astype(jnp.float32)
            for o in range(1, 3):
                total = total + band[t, o].astype(jnp.float32)
            for c in range(0, far_rows, lane):
                total = total + weights[:, c : c + lane]
            degree = jnp.sum(total, axis=1, keepdims=True)
            seeded = jnp.broadcast_to(seed_ref[pl.ds(t, 1), :].astype(jnp.float32), (tile, tile)).T
            inverse = jnp.broadcast_to(1.0 / degree, (tile, tile))
            inv[pl.ds(base, tile), :] = jnp.where(seeded == 1.0, -inverse, inverse)

    def out_copy(p):
        base = p * (2 * tile // GROUP)
        return pltpu.make_async_copy(
            cur[ITERS % 2].at[pl.ds(base + tile // GROUP, 2 * tile // GROUP)],
            out_hbm.at[pl.ds(base, 2 * tile // GROUP)],
            out_sem,
        )

    pairs = tiles // 2
    copies = halo_first
    for it in range(ITERS):
        exchange(it)
        if it == 0:
            farw_copy.wait()
            band_copy.wait()
            prepare()
        band_pass(it, 1, pairs - 1)
        await_halo(it, copies)
        band_pass(it, 0, 1)
        band_pass(it, pairs - 1, pairs)
        await_blocks(it)

        last = it == ITERS - 1
        if not last:
            copies = halo_copies(
                it + 1, cur[it + 1].at[groups(tile, tile)], cur[it + 1].at[groups(rows, tile)]
            )

        def pair_at(i):
            return lax.rem(i + pairs - 1, pairs)

        far_pass(it, pair_at(0), far_a)

        @pl.loop(0, pairs // 2)
        def _(q):
            far_pass(it, pair_at(2 * q + 1), far_b)
            finish(it, pair_at(2 * q), far_a)
            far_pass(it, pair_at(2 * q + 2), far_a)
            finish(it, pair_at(2 * q + 1), far_b)
            if last:

                @pl.when(q > 0)
                def _():
                    out_copy(pair_at(2 * q - 2)).start()
                    out_copy(pair_at(2 * q - 1)).start()

            else:

                @pl.when(q == 1)
                def _():
                    for copy in copies:
                        copy.start()

        sums = jnp.sum(part[...], axis=1)
        res_ref[it : it + 1, :] = jnp.sum(sums.T, axis=0, keepdims=True)

    out_copy(pairs - 3).start()
    out_copy(pairs - 2).start()
    whole = pltpu.make_async_copy(cur[ITERS % 2].at[groups(tile, rows)], out_hbm, out_sem)
    whole.wait()
    both = pl.ds(0, n - 1)
    pltpu.make_async_copy(req_in.at[both], req_in.at[both], req_send).wait()


def body(labels, seed_mask, band_w, far_block, far_tile, far_count, far_w):
    rows, classes = labels.shape
    tiles, _, tile, _ = band_w.shape
    _, n, slots, blk, _ = far_w.shape
    lane = 128
    per = slots * blk
    dims = (n, tiles, tile, slots, blk, classes)
    vmem, anywhere = pltpu.VMEM, pl.BlockSpec(memory_space=pl.ANY)
    held = pl.BlockSpec(memory_space=pltpu.VMEM)
    dma = pltpu.SemaphoreType.DMA
    bf16, f32 = jnp.bfloat16, jnp.float32
    out, residual = pl.pallas_call(
        functools.partial(kernel, dims),
        out_shape=(
            jax.ShapeDtypeStruct((rows // GROUP, GROUP, classes), bf16),
            jax.ShapeDtypeStruct((ITERS, tiles), f32),
        ),
        in_specs=[anywhere, anywhere, anywhere, held, held, held, held],
        out_specs=(anywhere, held),
        scratch_shapes=[
            vmem(((rows + 2 * tile) // GROUP, GROUP, classes), bf16),
            vmem(((rows + 2 * tile) // GROUP, GROUP, classes), bf16),
            vmem(band_w.shape, bf16),
            vmem((n * per, tile), bf16),
            vmem((tile, n * per), f32),
            vmem((tiles, n * per), f32),
            vmem((rows, n * per), bf16),
            vmem((rows, classes), f32),
            vmem((2 * tile, classes), f32),
            vmem((2 * tile, classes), f32),
            vmem((rows, lane), f32),
            vmem((tiles, 8, lane), f32),
            vmem((2, tile // GROUP, GROUP, classes), bf16),
            vmem((2, tile // GROUP, GROUP, classes), bf16),
            vmem((n, per, classes), bf16),
            vmem((n, per, classes), bf16),
            vmem((n, per, classes), bf16),
            vmem((n, per, classes), bf16),
            vmem((n, slots, n), jnp.int32),
            pltpu.SMEM((n, slots, n), jnp.int32),
            dma, dma, dma, dma, dma,
            dma, dma,
            dma((ITERS, 2)), dma((ITERS, 2)),
            dma((ITERS,)), dma((ITERS,)),
        ],
        compiler_params=pltpu.CompilerParams(
            collective_id=0, has_side_effects=True, vmem_limit_bytes=60 * 1024 * 1024
        ),
    )(
        labels.reshape(rows // GROUP, GROUP, classes),
        band_w,
        far_w.reshape(n * per, tile),
        far_block[0].T,
        far_tile[0].T,
        far_count,
        seed_mask.reshape(tiles, tile),
    )
    return out.reshape(rows, classes), residual


def solution(mesh):
    placed = (
        P("node", None),
        P("node"),
        P("node", None, None, None),
        P("node", None, None),
        P("node", None, None),
        P("node", None),
        P("node", None, None, None, None),
    )
    return jax.shard_map(
        body,
        mesh=mesh,
        in_specs=placed,
        out_specs=(P("node", None), P(None, "node")),
        check_vma=False,
    )
```

```python
import functools

import jax
import jax.numpy as jnp
from jax import lax
from jax.experimental import pallas as pl
from jax.experimental.pallas import tpu as pltpu
from jax.sharding import PartitionSpec as P

ITERS = 2
MESH = pl.DeviceIdType.MESH
ROWS = 32
GROUP = 16


def kernel(
    dims,
    labels_hbm, band_hbm, farw_hbm, req_ref, tile_ref, count_ref, seed_ref,
    out_ref, res_ref,
    cur0, cur1, band, farw, wide_t, onehot, placed, acc, far_a, far_b, inv, part,
    halo0, halo1, send0, send1, recv0, recv1, req_in, req_s,
    lab_sem, band_sem, farw_sem, smem_sem,
    req_send, req_recv, halo_send, halo_recv, blk_send, blk_recv,
):
    n, tiles, tile, slots, blk, classes = dims
    rows = tiles * tile
    lane = 128
    per = slots * blk
    far_rows = n * per
    me = lax.axis_index("node")
    right, left = lax.rem(me + 1, n), lax.rem(me + n - 1, n)
    cur = (cur0, cur1)
    halo, send, recv = (halo0, halo1), (send0, send1), (recv0, recv1)

    def groups(start, size):
        return pl.ds(start // GROUP, size // GROUP)

    def as_rows(value):
        return value.reshape(-1, classes)

    lab_copy = pltpu.make_async_copy(labels_hbm, cur0.at[groups(tile, rows)], lab_sem)
    band_copy = pltpu.make_async_copy(band_hbm, band, band_sem)
    farw_copy = pltpu.make_async_copy(farw_hbm, farw, farw_sem)
    lab_copy.start()
    farw_copy.start()
    band_copy.start()

    barrier = pltpu.get_barrier_semaphore()

    @pl.loop(1, n)
    def _(j):
        pl.semaphore_signal(barrier, inc=1, device_id=(lax.rem(me + j, n),), device_id_type=MESH)

    pl.semaphore_wait(barrier, n - 1)

    @pl.loop(1, n)
    def _(j):
        peer = lax.rem(me + j, n)
        pltpu.make_async_remote_copy(
            req_ref, req_in.at[me], req_send, req_recv,
            device_id=(peer,), device_id_type=MESH,
        ).start()

    def halo_copies(it, low, high):
        return (
            pltpu.make_async_remote_copy(
                high, halo[it].at[0], halo_send.at[it, 0], halo_recv.at[it, 0],
                device_id=(right,), device_id_type=MESH,
            ),
            pltpu.make_async_remote_copy(
                low, halo[it].at[1], halo_send.at[it, 1], halo_recv.at[it, 1],
                device_id=(left,), device_id_type=MESH,
            ),
        )

    halo_first = halo_copies(
        0, labels_hbm.at[groups(0, tile)], labels_hbm.at[groups(rows - tile, tile)]
    )
    for copy in halo_first:
        copy.start()

    req_in[me] = req_ref[...]
    lab_copy.wait()
    pltpu.make_async_copy(req_in.at[pl.ds(0, n - 1)], req_in.at[pl.ds(0, n - 1)], req_recv).wait()
    smem_copy = pltpu.make_async_copy(req_in, req_s, smem_sem)
    smem_copy.start()
    smem_copy.wait()

    def block_copy(it, j):
        peer = lax.rem(me + j, n)
        return pltpu.make_async_remote_copy(
            send[it].at[peer], recv[it].at[me], blk_send.at[it], blk_recv.at[it],
            device_id=(peer,), device_id_type=MESH,
        )

    def gathered(it, peer):
        halves = []
        for k in range(slots):
            wanted = req_s[peer, k, me]
            pair = cur[it][wanted // 2 + tile // GROUP].astype(jnp.float32)
            odd = jnp.full((blk, classes), wanted % 2, jnp.int32) == 1
            halves.append(jnp.where(odd, pair[blk:], pair[:blk]))
        return jnp.concatenate(halves, axis=0).astype(jnp.bfloat16)

    def exchange(it):
        @pl.loop(1, n)
        def _(j):
            peer = lax.rem(me + j, n)
            send[it][peer] = gathered(it, peer)

            @pl.when(j > 1)
            def _():
                block_copy(it, j - 1).start()

        recv[it][me] = gathered(it, me)
        block_copy(it, n - 1).start()

    def await_halo(it, copies):
        for copy in copies:
            copy.wait()
        cur[it][groups(0, tile)] = halo[it][0]
        cur[it][groups(rows + tile, tile)] = halo[it][1]

    def await_blocks(it):
        both = pl.ds(0, n - 1)
        pltpu.make_async_copy(send[it].at[both], send[it].at[both], blk_send.at[it]).wait()
        pltpu.make_async_copy(recv[it].at[both], recv[it].at[both], blk_recv.at[it]).wait()

    def band_pass(it, start, stop):
        zero = jnp.zeros((tile, tile), jnp.bfloat16)

        @pl.loop(start, stop)
        def _(p):
            first = [band[2 * p, o] for o in range(3)]
            second = [band[2 * p + 1, o] for o in range(3)]
            weights = jnp.concatenate(
                [jnp.concatenate(first + [zero], axis=1), jnp.concatenate([zero] + second, axis=1)],
                axis=0,
            )
            base = pl.multiple_of(p * (2 * tile), 2 * tile)
            acc[pl.ds(base, 2 * tile), :] = jnp.dot(
                weights,
                as_rows(cur[it][pl.ds(p * (2 * tile // GROUP), 4 * tile // GROUP)]),
                preferred_element_type=jnp.float32,
            )

    def far_pass(it, p, into):
        base = pl.multiple_of(p * (2 * tile), 2 * tile)
        into[...] = jnp.dot(
            placed[pl.ds(base, 2 * tile), :],
            recv[it][...].reshape(far_rows, classes),
            preferred_element_type=jnp.float32,
        )

    def finish(it, p, far):
        last = it == ITERS - 1
        target = out_ref if last else cur[1 - it]
        for half in range(2):
            total = jnp.zeros((8, lane), jnp.float32)
            for r in range(0, tile, ROWS):
                base = pl.multiple_of(p * (2 * tile) + half * tile + r, ROWS)
                here = pl.ds(base, ROWS)
                local = slice(half * tile + r, half * tile + r + ROWS)
                spread = [
                    acc[here, c : c + lane] + far[local, c : c + lane]
                    for c in range(0, classes, lane)
                ]
                squares = spread[0] * spread[0]
                for s in spread[1:]:
                    squares = squares + s * s
                mean = jnp.sum(squares, axis=1, keepdims=True) * (1.0 / classes)
                signed = inv[here, :]
                size = jnp.abs(signed)
                factor = size / jnp.maximum(size * jnp.sqrt(mean), 0.05)
                keep = signed < 0.0
                padded = pl.ds(
                    p * (2 * tile // GROUP) + (half * tile + r + tile) // GROUP, ROWS // GROUP
                )
                written = pl.ds(padded.start - tile // GROUP, padded.size) if last else padded
                for q, s in enumerate(spread):
                    where = slice(q * lane, (q + 1) * lane)
                    before = cur[it][padded, :, where].reshape(ROWS, lane).astype(jnp.float32)
                    fresh = jnp.where(keep, before, s * factor).astype(jnp.bfloat16)
                    target[written, :, where] = fresh.reshape(ROWS // GROUP, GROUP, lane)
                    change = jnp.abs(fresh.astype(jnp.float32) - before)
                    for i in range(0, ROWS, 8):
                        total = total + change[i : i + 8]
            part[2 * p + half] = total

    def prepare():
        wide_t[...] = farw[...].astype(jnp.float32).T
        tile_of = lax.broadcasted_iota(jnp.int32, (tiles, n), 0)
        block_of = lax.shift_right_logical(
            lax.broadcasted_iota(jnp.int32, (n, far_rows), 1), blk.bit_length() - 1
        )
        peer_of = lax.broadcasted_iota(jnp.int32, (n, far_rows), 0)
        table = jnp.zeros((tiles, far_rows), jnp.float32)
        for k in range(slots):
            target = jnp.where(count_ref[...] > k, tile_ref[k : k + 1, :], -1)
            chosen = (tile_of == target).astype(jnp.float32)
            spread = (block_of == peer_of * slots + k).astype(jnp.float32)
            table = table + jnp.dot(
                chosen.astype(jnp.bfloat16),
                spread.astype(jnp.bfloat16),
                preferred_element_type=jnp.float32,
            )
        onehot[...] = table

        @pl.loop(0, tiles)
        def _(t):
            base = pl.multiple_of(t * tile, tile)
            weights = wide_t[...] * onehot[pl.ds(t, 1), :]
            placed[pl.ds(base, tile), :] = weights.astype(jnp.bfloat16)
            total = band[t, 0].astype(jnp.float32)
            for o in range(1, 3):
                total = total + band[t, o].astype(jnp.float32)
            for c in range(0, far_rows, lane):
                total = total + weights[:, c : c + lane]
            degree = jnp.sum(total, axis=1, keepdims=True)
            seeded = jnp.broadcast_to(seed_ref[pl.ds(t, 1), :].astype(jnp.float32), (tile, tile)).T
            inverse = jnp.broadcast_to(1.0 / degree, (tile, tile))
            inv[pl.ds(base, tile), :] = jnp.where(seeded == 1.0, -inverse, inverse)

    pairs = tiles // 2
    copies = halo_first
    for it in range(ITERS):
        exchange(it)
        if it == 0:
            farw_copy.wait()
            band_copy.wait()
            prepare()
        band_pass(it, 1, pairs - 1)
        await_halo(it, copies)
        band_pass(it, 0, 1)
        band_pass(it, pairs - 1, pairs)
        await_blocks(it)

        last = it == ITERS - 1
        if not last:
            copies = halo_copies(
                it + 1, cur[it + 1].at[groups(tile, tile)], cur[it + 1].at[groups(rows, tile)]
            )

        def pair_at(i):
            return lax.rem(i + pairs - 1, pairs)

        far_pass(it, pair_at(0), far_a)

        @pl.loop(0, pairs // 2)
        def _(q):
            far_pass(it, pair_at(2 * q + 1), far_b)
            finish(it, pair_at(2 * q), far_a)
            far_pass(it, pair_at(2 * q + 2), far_a)
            finish(it, pair_at(2 * q + 1), far_b)
            if not last:

                @pl.when(q == 1)
                def _():
                    for copy in copies:
                        copy.start()

        sums = jnp.sum(part[...], axis=1)
        res_ref[it : it + 1, :] = jnp.sum(sums.T, axis=0, keepdims=True)

    both = pl.ds(0, n - 1)
    pltpu.make_async_copy(req_in.at[both], req_in.at[both], req_send).wait()


def body(labels, seed_mask, band_w, far_block, far_tile, far_count, far_w):
    rows, classes = labels.shape
    tiles, _, tile, _ = band_w.shape
    _, n, slots, blk, _ = far_w.shape
    lane = 128
    per = slots * blk
    dims = (n, tiles, tile, slots, blk, classes)
    vmem, anywhere = pltpu.VMEM, pl.BlockSpec(memory_space=pl.ANY)
    held = pl.BlockSpec(memory_space=pltpu.VMEM)
    dma = pltpu.SemaphoreType.DMA
    bf16, f32 = jnp.bfloat16, jnp.float32
    out, residual = pl.pallas_call(
        functools.partial(kernel, dims),
        out_shape=(
            pltpu.VMEM((rows // GROUP, GROUP, classes), bf16),
            jax.ShapeDtypeStruct((ITERS, tiles), f32),
        ),
        in_specs=[anywhere, anywhere, anywhere, held, held, held, held],
        out_specs=(held, held),
        scratch_shapes=[
            vmem(((rows + 2 * tile) // GROUP, GROUP, classes), bf16),
            vmem(((rows + 2 * tile) // GROUP, GROUP, classes), bf16),
            vmem(band_w.shape, bf16),
            vmem((n * per, tile), bf16),
            vmem((tile, n * per), f32),
            vmem((tiles, n * per), f32),
            vmem((rows, n * per), bf16),
            vmem((rows, classes), f32),
            vmem((2 * tile, classes), f32),
            vmem((2 * tile, classes), f32),
            vmem((rows, lane), f32),
            vmem((tiles, 8, lane), f32),
            vmem((2, tile // GROUP, GROUP, classes), bf16),
            vmem((2, tile // GROUP, GROUP, classes), bf16),
            vmem((n, per, classes), bf16),
            vmem((n, per, classes), bf16),
            vmem((n, per, classes), bf16),
            vmem((n, per, classes), bf16),
            vmem((n, slots, n), jnp.int32),
            pltpu.SMEM((n, slots, n), jnp.int32),
            dma, dma, dma, dma,
            dma, dma,
            dma((ITERS, 2)), dma((ITERS, 2)),
            dma((ITERS,)), dma((ITERS,)),
        ],
        compiler_params=pltpu.CompilerParams(
            collective_id=0, has_side_effects=True, vmem_limit_bytes=56 * 1024 * 1024
        ),
    )(
        labels.reshape(rows // GROUP, GROUP, classes),
        band_w,
        far_w.reshape(n * per, tile),
        far_block[0].T,
        far_tile[0].T,
        far_count,
        seed_mask.reshape(tiles, tile),
    )
    return out.reshape(rows, classes), residual


def solution(mesh):
    placed = (
        P("node", None),
        P("node"),
        P("node", None, None, None),
        P("node", None, None),
        P("node", None, None),
        P("node", None),
        P("node", None, None, None, None),
    )
    return jax.shard_map(
        body,
        mesh=mesh,
        in_specs=placed,
        out_specs=(P("node", None), P(None, "node")),
        check_vma=False,
    )
```
